32 devices in a mesh: node: 4 (over y, x), torus: 8 (over z, core).
Axes of the slice: x: 2, y: 2, z: 4, core: 2. Of those that a mesh axis runs over, the one named last changes fastest.
Arguments:
- tokens: bfloat16 [4096, 7168], P(('node', 'torus')), may hold values from -6 to 6
- expert_ids: int32 [4096, 8], P(('node', 'torus')), may hold values from 0 to 383, as said below
- route_weight: bfloat16 [4096, 8], P(('node', 'torus')), may hold values from 0.19921875 to 2.5
- w_gate: bfloat16 [16, 7168, 1024], P('torus', None, 'node'), may hold values from -0.0625 to 0.0625
- w_up: bfloat16 [16, 7168, 1024], P('torus', None, 'node'), may hold values from -0.0625 to 0.0625
- w_down: bfloat16 [16, 1024, 7168], P('torus', 'node'), may hold values from -0.1875 to 0.1875
Outputs:
- moe_out: bfloat16 [4096, 7168], P(('node', 'torus'))
The draws below stay inside these ranges and needn't reach their ends.
Inputs may be any that keep to these rules, and one draw needn't show every extreme that they name: `expert_ids`: each row names 8 different experts. Counting an expert e below 16 as one of group e // 2, at most 4 of the 128 rows of one device (aligned blocks of rows, in order) name an expert of any one group, and in every draw some group is named by exactly 4 rows of every device.
All inputs are finite; a program needn't handle non-finite values.
Results may differ from the reference program's by a relative error of at most 0.0095.
Values may be sent and summed in bfloat16 or wider, within the bound.
A program may use at most 128 MiB of HBM per device.

```python
import math
import jax
import jax.numpy as jnp
from jax import lax

D = 7168
FF = 1024
EXPERTS = 384
TOPK = 8
EXP_DEV = 2
CAP = 4
QBLOCK = 128
TOK_DEV = 128
GROUPS = 8
SOURCES = 32
WIN_EXPERTS = 16
TOKENS = 4096
N_NODE = 4


def draw_expert_ids(key, part):
    keys = jax.random.split(jax.random.fold_in(key, 17), 8)
    group_ids = jnp.arange(GROUPS, dtype=jnp.int32)
    hot_group = jax.random.randint(keys[0], (), 0, GROUPS, dtype=jnp.int32)
    second_group = jax.random.randint(keys[1], (SOURCES,), 0, GROUPS, dtype=jnp.int32)
    second_used = jax.random.randint(keys[2], (SOURCES,), 0, 2, dtype=jnp.int32)
    counts = jax.random.randint(keys[3], (SOURCES, GROUPS), 1, 4, dtype=jnp.int32)
    counts = jnp.where(group_ids[None, :] == hot_group, CAP, counts)
    counts = jnp.where((group_ids[None, :] == second_group[:, None]) & (second_used[:, None] == 1), CAP, counts)
    ends = jnp.cumsum(counts, axis=1).astype(jnp.int32)
    laps = TOPK // EXP_DEV
    position = jnp.arange(laps * TOK_DEV, dtype=jnp.int32).reshape(laps, TOK_DEV)
    owner = jnp.sum((ends[:, None, None, :] <= position[None, :, :, None]).astype(jnp.int32), axis=-1)
    inside = position[None, :, :] < ends[:, -1][:, None, None]
    picked = jax.random.randint(keys[4], (SOURCES, laps, TOK_DEV), 0, 3, dtype=jnp.int32)
    first = EXP_DEV * owner + (picked == 1).astype(jnp.int32)
    second = EXP_DEV * owner + 1
    first = jnp.where(inside, first, -1)
    second = jnp.where(inside & (picked == 2), second, -1)
    paired = jnp.stack([first, second], axis=2)
    slots = paired.reshape(SOURCES, TOPK, TOK_DEV).transpose(0, 2, 1)
    shuffles = jax.vmap(lambda sub: jax.random.permutation(sub, TOK_DEV))(jax.random.split(keys[5], SOURCES))
    inverse = jnp.argsort(shuffles, axis=1).astype(jnp.int32)
    slots = jnp.take_along_axis(slots, inverse[:, :, None], axis=1)
    remain = EXPERTS - WIN_EXPERTS
    offset = jax.random.randint(keys[6], (SOURCES, TOK_DEV, 1), 0, remain, dtype=jnp.int32)
    filler = WIN_EXPERTS + (offset + jnp.arange(TOPK, dtype=jnp.int32)[None, None, :]) % remain
    chosen = jnp.where(slots >= 0, slots, filler)
    scores = jax.random.randint(keys[7], (SOURCES, TOK_DEV, TOPK), 0, 1 << 20, dtype=jnp.int32) * TOPK + jnp.arange(TOPK, dtype=jnp.int32)[None, None, :]
    order = jnp.argsort(scores, axis=-1, stable=True)
    chosen = jnp.take_along_axis(chosen, order, axis=-1)
    return chosen.reshape(TOKENS, TOPK).astype(jnp.int32)


def steps_of(stream_key, dims, cuts, least, high):
    gain, own = 1.0, jax.random.fold_in(stream_key, 6)
    for axis_at, shards_of in cuts:
        draws = jnp.exp(jax.random.uniform(jax.random.fold_in(own, axis_at), (shards_of,), jnp.float32, least / len(cuts), high / len(cuts)))
        gain = gain * jnp.repeat(draws, dims[axis_at] // shards_of).reshape([-1 if axis == axis_at else 1 for axis in range(len(dims))])
    return gain


def centred(stream_key, shape, width, bound, cuts=(), held_as=jnp.bfloat16):
    loudness = steps_of(stream_key, shape, cuts, -0.22, 0.18) if cuts else 1.0
    drawn = jax.random.normal(stream_key, shape, jnp.float32) * width * loudness
    return jnp.minimum(jnp.maximum(drawn, -bound), bound).astype(held_as)


def setup_inputs(seed: int = 0) -> dict:
    streams_of = jax.random.split(jax.random.key(seed), 7)
    tokens = centred(streams_of[0], (TOKENS, D), 1.0, 6.0, ((0, 32),))
    expert_ids = draw_expert_ids(jax.random.fold_in(streams_of[6], 71), 0)
    route_weight = jnp.clip(jnp.exp(math.log(2.5) - 2.5296425 * jax.random.uniform(streams_of[2], (TOKENS, TOPK), jnp.float32) ** steps_of(streams_of[2], (TOKENS, TOPK), ((0, 32),), -0.2, 0.2)), 0.19921875, 2.5).astype(jnp.bfloat16)
    w_gate = centred(streams_of[3], (WIN_EXPERTS, D, FF), D ** -0.5, 0.0625, ((0, 8), (2, 4)))
    w_up = centred(streams_of[4], (WIN_EXPERTS, D, FF), D ** -0.5, 0.0625, ((0, 8), (2, 4)))
    w_down = centred(streams_of[5], (WIN_EXPERTS, FF, D), FF ** -0.5, 0.1875, ((0, 8), (1, 4)))
    return {"tokens": tokens, "expert_ids": expert_ids, "route_weight": route_weight, "w_gate": w_gate, "w_up": w_up, "w_down": w_down}


block_rows = 64


def quantize(tokens):
    count = tokens.shape[0]
    blocks = tokens.astype(jnp.float32).reshape(count, -1, QBLOCK)
    largest = jnp.max(jnp.abs(blocks), axis=-1)
    scale = ((largest + 1e-6) * (1.0 / 448.0)).astype(jnp.bfloat16)
    scale = lax.optimization_barrier(scale)
    quantized = (blocks / scale.astype(jnp.float32)[:, :, None]).astype(jnp.bfloat16)
    quantized = lax.optimization_barrier(quantized)
    return quantized.reshape(count, -1), scale


def restore(quantized, scale):
    count = quantized.shape[0]
    blocks = quantized.astype(jnp.float32).reshape(count, -1, QBLOCK) * scale.astype(jnp.float32)[:, :, None]
    return blocks.astype(jnp.bfloat16).reshape(count, -1)


def reference(tokens, expert_ids, route_weight, w_gate, w_up, w_down):
    quantized, scale = quantize(tokens)
    restored = restore(quantized, scale)
    experts = jnp.arange(WIN_EXPERTS, dtype=jnp.int32)
    weight_float = route_weight.astype(jnp.float32)
    route_sel = jnp.zeros((TOKENS, WIN_EXPERTS), jnp.float32)
    named = jnp.zeros((TOKENS, WIN_EXPERTS), jnp.int32)
    for slot in range(TOPK):
        matched = expert_ids[:, slot:slot + 1] == experts[None, :]
        route_sel = route_sel + jnp.where(matched, weight_float[:, slot:slot + 1], jnp.float32(0.0))
        named = named + matched.astype(jnp.int32)
    member = named.reshape(TOKENS, GROUPS, EXP_DEV).sum(axis=-1)
    route_sel = route_sel.reshape(TOKENS, GROUPS, EXP_DEV)
    quarter = FF // N_NODE
    total = jnp.zeros((TOKENS, D), jnp.float32)
    offsets = jnp.arange(block_rows, dtype=jnp.int32)

    def group_step(group, total):
        inside = lax.dynamic_index_in_dim(member, group, 1, keepdims=False) > 0
        count = jnp.sum(inside.astype(jnp.int32)).astype(jnp.int32)
        order = jnp.argsort(jnp.where(inside, 0, 1).astype(jnp.int32), stable=True).astype(jnp.int32)
        order = jnp.concatenate([order, jnp.zeros((block_rows,), jnp.int32)])
        weights_group = lax.dynamic_index_in_dim(route_sel, group, 1, keepdims=False)
        gates = [lax.dynamic_index_in_dim(w_gate, EXP_DEV * group + expert, 0, keepdims=False) for expert in range(EXP_DEV)]
        ups = [lax.dynamic_index_in_dim(w_up, EXP_DEV * group + expert, 0, keepdims=False) for expert in range(EXP_DEV)]
        downs = [lax.dynamic_index_in_dim(w_down, EXP_DEV * group + expert, 0, keepdims=False) for expert in range(EXP_DEV)]

        def block_step(block, total):
            start = (block * block_rows).astype(jnp.int32)
            picked = lax.dynamic_slice_in_dim(order, start, block_rows)
            valid = (start + offsets) < count
            rows = restored[picked]
            weights = weights_group[picked]
            parts = [jnp.zeros((block_rows, D), jnp.float32) for piece in range(N_NODE)]
            for expert in range(EXP_DEV):
                gate = jnp.dot(rows, gates[expert], preferred_element_type=jnp.float32)
                upper = jnp.dot(rows, ups[expert], preferred_element_type=jnp.float32)
                hidden = (jax.nn.silu(gate) * upper).astype(jnp.bfloat16)
                for piece in range(N_NODE):
                    lower = piece * quarter
                    result = jnp.dot(hidden[:, lower:lower + quarter], downs[expert][lower:lower + quarter, :], preferred_element_type=jnp.float32)
                    parts[piece] = parts[piece] + weights[:, expert:expert + 1] * result
            combined = jnp.zeros((block_rows, D), jnp.float32)
            for piece in range(N_NODE):
                rounded = lax.optimization_barrier(parts[piece].astype(jnp.bfloat16))
                combined = combined + rounded.astype(jnp.float32)
            combined = lax.optimization_barrier(combined.astype(jnp.bfloat16))
            added = jnp.where(valid[:, None], combined.astype(jnp.float32), jnp.float32(0.0))
            return total.at[picked].add(added)

        blocks = (count + block_rows - 1) // block_rows
        return lax.fori_loop(0, blocks, block_step, total)

    total = lax.fori_loop(0, GROUPS, group_step, total)
    return total.astype(jnp.bfloat16)
```

```python
import functools

import jax
import jax.numpy as jnp
from jax import lax
from jax.experimental import pallas as pl
from jax.experimental.pallas import tpu as pltpu
from jax.sharding import PartitionSpec as P

CAP = 4
QBLOCK = 128
PARTS = 4
SUB = CAP * PARTS
CHUNK = 1024
WIDE = CHUNK // PARTS
MESH = pl.DeviceIdType.MESH
F32 = jnp.float32
BF16 = jnp.bfloat16


def flipped(index, mask):
    value = index
    bit = 0
    while mask >> bit:
        if (mask >> bit) & 1:
            size = 1 << bit
            value = value + size * (1 - 2 * lax.rem(lax.div(index, jnp.int32(size)), jnp.int32(2)))
        bit += 1
    return value


def dot(left, right):
    return jnp.dot(left, right, preferred_element_type=F32)


def kernel(
    groups, chunks, lags,
    tok_hbm, ids_ref, rw_ref, wg_hbm, wu_hbm, wd_hbm, out_hbm,
    tok, wg, wu, wd, place, place_t, perm, perm_t,
    sent, held, wsent, wheld, xs, acc, hidden, wcol,
    part, relay_a, relay_b, got_x, got_y, back_s, back, obuf,
    sems, lsems,
):
    node = lax.axis_index("node")
    torus = lax.axis_index("torus")
    rows = tok.shape[0]
    subs = groups * SUB
    slots = groups * CAP
    half = slots // 2
    shalf = subs // 2
    units = subs // 128
    experts = wg.shape[0]
    at_x = (flipped(node, 1), torus)
    at_y = (flipped(node, 2), torus)
    at_z = [(node, flipped(torus, j)) for j in range(groups)]

    tok_cp, wg_cp, wu_cp, wd_cp = [], [], [], []
    for k in range(chunks):
        cols = pl.ds(k * CHUNK, CHUNK)
        tok_cp.append(pltpu.make_async_copy(tok_hbm.at[:, cols], tok.at[:, cols], lsems.at[0, k]))
        wg_cp.append(pltpu.make_async_copy(wg_hbm.at[:, cols, :], wg.at[:, cols, :], lsems.at[1, k]))
        wu_cp.append(pltpu.make_async_copy(wu_hbm.at[:, cols, :], wu.at[:, cols, :], lsems.at[2, k]))
        wd_cp.append(pltpu.make_async_copy(wd_hbm.at[:, :, cols], wd.at[:, :, cols], lsems.at[3, k]))
    for c in tok_cp:
        c.start()
    for a, b in zip(wg_cp, wu_cp):
        a.start()
        b.start()
    for c in wd_cp:
        c.start()

    barrier = pltpu.get_barrier_semaphore()
    for peer in at_z[1:] + [at_x, at_y]:
        pl.semaphore_signal(barrier, inc=1, device_id=peer, device_id_type=MESH)

    col = lax.broadcasted_iota(jnp.int32, (rows, subs), 1)
    gid = jnp.bitwise_xor(col // SUB, jnp.full((rows, subs), torus, jnp.int32))
    slot_of = (col // PARTS) % CAP
    part_of = col % PARTS
    hit = jnp.zeros((rows, subs), F32)
    chosen = [jnp.zeros((rows, subs), F32) for _ in range(experts)]
    for k in range(ids_ref.shape[1]):
        named = jnp.broadcast_to(ids_ref[:, k : k + 1], (rows, subs))
        weight = jnp.broadcast_to(rw_ref[:, k : k + 1], (rows, subs))
        for e in range(experts):
            same = named == gid * experts + e
            hit = jnp.where(same, 1.0, hit)
            chosen[e] = jnp.where(same, weight, chosen[e])
    lower = lax.broadcasted_iota(jnp.int32, (rows, rows), 1) < lax.broadcasted_iota(
        jnp.int32, (rows, rows), 0
    )
    before = dot(lower.astype(F32).astype(BF16), hit.astype(BF16))
    onehot = jnp.where(before == slot_of.astype(F32), hit, 0.0)
    for q in range(PARTS):
        mine = jnp.where(part_of == q, onehot, 0.0)
        place_t[q] = mine.astype(BF16)
        place[q] = mine.T.astype(BF16)
    lane = lax.broadcasted_iota(jnp.int32, (subs, 128), 1)
    wrow = jnp.zeros((subs, 128), F32)
    for e in range(experts):
        total = jnp.sum((onehot * chosen[e]).T, axis=1, keepdims=True)
        wrow = jnp.where(lane == e, total, wrow)
    wsent[...] = wrow.astype(BF16)
    wheld[0, 0:SUB] = wrow[0:SUB].astype(BF16)
    pr = lax.broadcasted_iota(jnp.int32, (128, 128), 0)
    pc = lax.broadcasted_iota(jnp.int32, (128, 128), 1)
    ur = 128 // PARTS
    perm[...] = (pc == (pr % ur) * PARTS + pr // ur).astype(F32).astype(BF16)
    perm_t[...] = (pr == (pc % ur) * PARTS + pc // ur).astype(F32).astype(BF16)

    pl.semaphore_wait(barrier, groups + 1)

    def remote(src, dst, a, b, k, peer):
        copy = pltpu.make_async_remote_copy(
            src_ref=src, dst_ref=dst, send_sem=sems.at[a, k], recv_sem=sems.at[b, k],
            device_id=peer, device_id_type=MESH,
        )
        copy.start()

    def wait(ref, a, k):
        pltpu.make_async_copy(ref, ref, sems.at[a, k]).wait()

    def views(k):
        if k == chunks:
            return wsent, wheld
        return sent.at[k], held.at[k]

    def exchange(k):
        src, dst = views(k)
        for j in range(1, groups):
            at = pl.ds(j * SUB, SUB)
            remote(src.at[at], dst.at[0, at], 0, 1, k, at_z[j])

    def spread(k):
        _, dst = views(k)
        wait(dst.at[0, pl.ds(SUB, subs - SUB)], 1, k)
        remote(dst.at[0], dst.at[1], 2, 3, k, at_x)
        remote(dst.at[0], dst.at[2], 4, 5, k, at_y)

    def forward(k):
        _, dst = views(k)
        wait(dst.at[1], 3, k)
        remote(dst.at[1, pl.ds(0, shalf)], dst.at[3, pl.ds(0, shalf)], 6, 7, k, at_y)
        wait(dst.at[2], 5, k)
        remote(dst.at[2, pl.ds(shalf, shalf)], dst.at[3, pl.ds(shalf, shalf)], 8, 9, k, at_x)

    def arrived(k):
        _, dst = views(k)
        wait(dst.at[3, pl.ds(0, shalf)], 7, k)
        wait(dst.at[3, pl.ds(shalf, shalf)], 9, k)

    def make(k):
        tok_cp[k].wait()
        picked = jnp.zeros((subs, WIDE), F32)
        for q in range(PARTS):
            picked += dot(place[q], tok[:, k * CHUNK + q * WIDE : k * CHUNK + (q + 1) * WIDE])
        for b in range(WIDE // QBLOCK):
            block = picked[:, b * QBLOCK : (b + 1) * QBLOCK]
            largest = jnp.max(jnp.abs(block), axis=1, keepdims=True)
            scale = ((largest + 1e-06) * (1.0 / 448.0)).astype(BF16).astype(F32)
            coded = (block / scale).astype(BF16).astype(F32)
            value = (coded * scale).astype(BF16)
            sent[k, :, b * QBLOCK : (b + 1) * QBLOCK] = value
            held[k, 0, 0:SUB, b * QBLOCK : (b + 1) * QBLOCK] = value[0:SUB]

    def unit_rows(r, u):
        return r * slots + u * ur

    def multiply(k):
        for r in range(4):
            for u in range(units):
                moved = dot(perm[...], held[k, r, u * 128 : (u + 1) * 128, :]).astype(BF16)
                at = unit_rows(r, u)
                for q in range(PARTS):
                    xs[at : at + ur, q * WIDE : (q + 1) * WIDE] = moved[q * ur : (q + 1) * ur]
        wg_cp[k].wait()
        wu_cp[k].wait()
        cols = pl.ds(k * CHUNK, CHUNK)
        for e in range(experts):
            for s, w in enumerate((wg, wu)):
                got = dot(xs[...], w[e, cols, :])
                if k == 0:
                    acc[e, s] = got
                else:
                    acc[e, s] += got

    exchange(chunks)
    l2, l3, l4 = lags
    for step in range(chunks + l4):
        if step < chunks:
            make(step)
            exchange(step)
        if step == l2:
            spread(chunks)
        if 0 <= step - l2 < chunks:
            spread(step - l2)
        if step == l3:
            forward(chunks)
        if 0 <= step - l3 < chunks:
            forward(step - l3)
        if step == l4:
            arrived(chunks)
            for r in range(4):
                for u in range(units):
                    moved = dot(perm[...], wheld[r, u * 128 : (u + 1) * 128, :])
                    at = unit_rows(r, u)
                    wcol[at : at + ur, :] = moved[0:ur]
        if 0 <= step - l4 < chunks:
            arrived(step - l4)
            multiply(step - l4)

    for e in range(experts):
        gate = acc[e, 0]
        hidden[e] = (gate / (1.0 + jnp.exp(-gate)) * acc[e, 1]).astype(BF16)

    def down(k):
        wd_cp[k].wait()
        for r in range(4):
            at = pl.ds(r * slots, slots)
            total = jnp.zeros((slots, CHUNK), F32)
            for e in range(experts):
                got = dot(hidden[e, at, :], wd[e, :, k * CHUNK : (k + 1) * CHUNK])
                total += wcol[at, e : e + 1] * got
            part[k, r] = total.astype(BF16)
        remote(part.at[k, 3, pl.ds(0, half)], relay_a.at[k], 10, 11, k, at_y)
        remote(part.at[k, 3, pl.ds(half, half)], relay_b.at[k], 12, 13, k, at_x)

    def merge(k):
        wait(relay_a.at[k], 11, k)
        part[k, 1, 0:half] = (part[k, 1, 0:half].astype(F32) + relay_a[k].astype(F32)).astype(BF16)
        remote(part.at[k, 1], got_x.at[k], 14, 15, k, at_x)
        wait(relay_b.at[k], 13, k)
        part[k, 2, half:slots] = (
            part[k, 2, half:slots].astype(F32) + relay_b[k].astype(F32)
        ).astype(BF16)
        remote(part.at[k, 2], got_y.at[k], 16, 17, k, at_y)

    def home(k):
        wait(got_x.at[k], 15, k)
        wait(got_y.at[k], 17, k)
        for u in range(units):
            at = pl.ds(u * ur, ur)
            total = (
                part[k, 0, at].astype(F32) + got_x[k, at].astype(F32) + got_y[k, at].astype(F32)
            ).astype(BF16)
            stacked = jnp.concatenate(
                [total[:, q * WIDE : (q + 1) * WIDE] for q in range(PARTS)], axis=0
            )
            moved = dot(perm_t[...], stacked).astype(BF16)
            back_s[k, u * 128 : (u + 1) * 128] = moved
            if u == 0:
                back[k, 0:SUB] = moved[0:SUB]
        for j in range(1, groups):
            at = pl.ds(j * SUB, SUB)
            remote(back_s.at[k, at], back.at[k, at], 18, 19, k, at_z[j])

    out_cp = [
        pltpu.make_async_copy(obuf.at[k], out_hbm.at[:, pl.ds(k * CHUNK, CHUNK)], lsems.at[4, k])
        for k in range(chunks)
    ]

    def finish(k):
        wait(back.at[k, pl.ds(SUB, subs - SUB)], 19, k)
        for q in range(PARTS):
            obuf[k, :, q * WIDE : (q + 1) * WIDE] = dot(place_t[q], back[k]).astype(BF16)
        out_cp[k].start()

    for step in range(chunks + l4):
        if step < chunks:
            down(step)
        if 0 <= step - l2 < chunks:
            merge(step - l2)
        if 0 <= step - l3 < chunks:
            home(step - l3)
        if 0 <= step - l4 < chunks:
            finish(step - l4)

    for k in range(chunks + 1):
        src, dst = views(k)
        wait(src.at[pl.ds(SUB, subs - SUB)], 0, k)
        wait(dst.at[0], 2, k)
        wait(dst.at[0], 4, k)
        wait(dst.at[1, pl.ds(0, shalf)], 6, k)
        wait(dst.at[2, pl.ds(shalf, shalf)], 8, k)
    for k in range(chunks):
        wait(relay_a.at[k], 10, k)
        wait(relay_b.at[k], 12, k)
        wait(got_x.at[k], 14, k)
        wait(got_y.at[k], 16, k)
        wait(back_s.at[k, pl.ds(SUB, subs - SUB)], 18, k)
        out_cp[k].wait()


LAGS = (1, 2, 3)


def shards(tokens, expert_ids, route_weight, w_gate, w_up, w_down):
    groups = lax.axis_size("torus")
    rows, width = tokens.shape
    experts, _, units = w_gate.shape
    chunks = width // CHUNK
    subs = groups * SUB
    slots = groups * CAP
    anywhere = pl.BlockSpec(memory_space=pl.ANY)
    local = pl.BlockSpec(memory_space=pltpu.VMEM)
    V = pltpu.VMEM
    return pl.pallas_call(
        functools.partial(kernel, groups, chunks, LAGS),
        out_shape=jax.ShapeDtypeStruct((rows, width), BF16),
        in_specs=[anywhere, local, local, anywhere, anywhere, anywhere],
        out_specs=anywhere,
        scratch_shapes=[
            V((rows, width), BF16),
            V(w_gate.shape, BF16),
            V(w_up.shape, BF16),
            V(w_down.shape, BF16),
            V((PARTS, subs, rows), BF16),
            V((PARTS, rows, subs), BF16),
            V((128, 128), BF16),
            V((128, 128), BF16),
            V((chunks, subs, WIDE), BF16),
            V((chunks, 4, subs, WIDE), BF16),
            V((subs, 128), BF16),
            V((4, subs, 128), BF16),
            V((4 * slots, CHUNK), BF16),
            V((experts, 2, 4 * slots, units), F32),
            V((experts, 4 * slots, units), BF16),
            V((4 * slots, 128), F32),
            V((chunks, 4, slots, CHUNK), BF16),
            V((chunks, slots // 2, CHUNK), BF16),
            V((chunks, slots // 2, CHUNK), BF16),
            V((chunks, slots, CHUNK), BF16),
            V((chunks, slots, CHUNK), BF16),
            V((chunks, subs, WIDE), BF16),
            V((chunks, subs, WIDE), BF16),
            V((chunks, rows, CHUNK), BF16),
            pltpu.SemaphoreType.DMA((20, chunks + 1)),
            pltpu.SemaphoreType.DMA((5, chunks)),
        ],
        compiler_params=pltpu.CompilerParams(
            collective_id=0, has_side_effects=True, vmem_limit_bytes=64000000
        ),
    )(tokens, expert_ids, route_weight.astype(F32), w_gate, w_up, w_down)


def solution(mesh):
    placed = (
        P(("node", "torus"), None),
        P(("node", "torus"), None),
        P(("node", "torus"), None),
        P("torus", None, "node"),
        P("torus", None, "node"),
        P("torus", "node", None),
    )
    return jax.shard_map(
        shards, mesh=mesh, in_specs=placed, out_specs=P(("node", "torus"), None), check_vma=False
    )
```

```python
import functools

import jax
import jax.numpy as jnp
from jax import lax
from jax.experimental import pallas as pl
from jax.experimental.pallas import tpu as pltpu
from jax.sharding import PartitionSpec as P

CAP = 4
QBLOCK = 128
PARTS = 4
SUB = CAP * PARTS
CHUNK = 1024
WIDE = CHUNK // PARTS
MESH = pl.DeviceIdType.MESH
F32 = jnp.float32
BF16 = jnp.bfloat16


def flipped(index, mask):
    value = index
    bit = 0
    while mask >> bit:
        if (mask >> bit) & 1:
            size = 1 << bit
            value = value + size * (1 - 2 * lax.rem(lax.div(index, jnp.int32(size)), jnp.int32(2)))
        bit += 1
    return value


def dot(left, right):
    return jnp.dot(left, right, preferred_element_type=F32)


def kernel(
    groups, chunks, lags,
    tok_hbm, ids_ref, rw_ref, wg_hbm, wu_hbm, wd_hbm, out_hbm,
    tok, wg, wu, wd, place, place_t, perm, perm_t,
    sent, held, wsent, wheld, xs, acc, hidden, wcol,
    part, relay_a, relay_b, got_x, got_y, back_s, back, obuf,
    sems, lsems,
):
    node = lax.axis_index("node")
    torus = lax.axis_index("torus")
    rows = tok.shape[0]
    subs = groups * SUB
    slots = groups * CAP
    half = slots // 2
    shalf = subs // 2
    units = subs // 128
    experts = wg.shape[0]
    at_x = (flipped(node, 1), torus)
    at_y = (flipped(node, 2), torus)
    at_z = [(node, flipped(torus, j)) for j in range(groups)]

    tok_cp, wg_cp, wu_cp, wd_cp = [], [], [], []
    for k in range(chunks):
        cols = pl.ds(k * CHUNK, CHUNK)
        tok_cp.append(pltpu.make_async_copy(tok_hbm.at[:, cols], tok.at[:, cols], lsems.at[0, k]))
        wg_cp.append(pltpu.make_async_copy(wg_hbm.at[:, cols, :], wg.at[:, cols, :], lsems.at[1, k]))
        wu_cp.append(pltpu.make_async_copy(wu_hbm.at[:, cols, :], wu.at[:, cols, :], lsems.at[2, k]))
        wd_cp.append(pltpu.make_async_copy(wd_hbm.at[:, :, cols], wd.at[:, :, cols], lsems.at[3, k]))
    for c in tok_cp:
        c.start()
    for a, b in zip(wg_cp, wu_cp):
        a.start()
        b.start()
    for c in wd_cp:
        c.start()

    barrier = pltpu.get_barrier_semaphore()
    for peer in at_z[1:] + [at_x, at_y]:
        pl.semaphore_signal(barrier, inc=1, device_id=peer, device_id_type=MESH)

    row = lax.broadcasted_iota(jnp.int32, (subs, rows), 0)
    gid = jnp.bitwise_xor(row // SUB, jnp.full((subs, rows), torus, jnp.int32))
    slot_of = (row // PARTS) % CAP
    part_of = row % PARTS
    hit = jnp.zeros((subs, rows), F32)
    chosen = [jnp.zeros((subs, rows), F32) for _ in range(experts)]
    weights = rw_ref[...].astype(F32)
    for k in range(ids_ref.shape[0]):
        named = jnp.broadcast_to(ids_ref[k : k + 1, :], (subs, rows))
        weight = jnp.broadcast_to(weights[k : k + 1, :], (subs, rows))
        for e in range(experts):
            same = named == gid * experts + e
            hit = jnp.where(same, 1.0, hit)
            chosen[e] = jnp.where(same, weight, chosen[e])
    lower = lax.broadcasted_iota(jnp.int32, (rows, rows), 0) < lax.broadcasted_iota(
        jnp.int32, (rows, rows), 1
    )
    before = dot(hit.astype(BF16), lower.astype(F32).astype(BF16))
    onehot = jnp.where(before == slot_of.astype(F32), hit, 0.0)
    lane = lax.broadcasted_iota(jnp.int32, (subs, 128), 1)
    wrow = jnp.zeros((subs, 128), F32)
    for e in range(experts):
        total = jnp.sum(onehot * chosen[e], axis=1, keepdims=True)
        wrow = jnp.where(lane == e, total, wrow)
    wsent[...] = wrow.astype(BF16)
    wheld[0, 0:SUB] = wrow[0:SUB].astype(BF16)
    for q in range(PARTS):
        place[q] = jnp.where(part_of == q, onehot, 0.0).astype(BF16)
    pr = lax.broadcasted_iota(jnp.int32, (128, 128), 0)
    pc = lax.broadcasted_iota(jnp.int32, (128, 128), 1)
    ur = 128 // PARTS
    perm[...] = (pc == (pr % ur) * PARTS + pr // ur).astype(F32).astype(BF16)
    perm_t[...] = (pr == (pc % ur) * PARTS + pc // ur).astype(F32).astype(BF16)

    pl.semaphore_wait(barrier, groups + 1)

    def remote(src, dst, a, b, k, peer):
        copy = pltpu.make_async_remote_copy(
            src_ref=src, dst_ref=dst, send_sem=sems.at[a, k], recv_sem=sems.at[b, k],
            device_id=peer, device_id_type=MESH,
        )
        copy.start()

    def wait(ref, a, k):
        pltpu.make_async_copy(ref, ref, sems.at[a, k]).wait()

    def views(k):
        if k == chunks:
            return wsent, wheld
        return sent.at[k], held.at[k]

    def exchange(k):
        src, dst = views(k)
        for j in range(1, groups):
            at = pl.ds(j * SUB, SUB)
            remote(src.at[at], dst.at[0, at], 0, 1, k, at_z[j])

    def spread(k):
        _, dst = views(k)
        wait(dst.at[0, pl.ds(SUB, subs - SUB)], 1, k)
        remote(dst.at[0], dst.at[1], 2, 3, k, at_x)
        remote(dst.at[0], dst.at[2], 4, 5, k, at_y)

    def forward(k):
        _, dst = views(k)
        wait(dst.at[1], 3, k)
        remote(dst.at[1, pl.ds(0, shalf)], dst.at[3, pl.ds(0, shalf)], 6, 7, k, at_y)
        wait(dst.at[2], 5, k)
        remote(dst.at[2, pl.ds(shalf, shalf)], dst.at[3, pl.ds(shalf, shalf)], 8, 9, k, at_x)

    def arrived(k):
        _, dst = views(k)
        wait(dst.at[3, pl.ds(0, shalf)], 7, k)
        wait(dst.at[3, pl.ds(shalf, shalf)], 9, k)

    def make(k):
        tok_cp[k].wait()
        picked = jnp.zeros((subs, WIDE), F32)
        for q in range(PARTS):
            picked += dot(place[q], tok[:, k * CHUNK + q * WIDE : k * CHUNK + (q + 1) * WIDE])
        for b in range(WIDE // QBLOCK):
            block = picked[:, b * QBLOCK : (b + 1) * QBLOCK]
            largest = jnp.max(jnp.abs(block), axis=1, keepdims=True)
            scale = ((largest + 1e-06) * (1.0 / 448.0)).astype(BF16).astype(F32)
            coded = (block / scale).astype(BF16).astype(F32)
            value = (coded * scale).astype(BF16)
            sent[k, :, b * QBLOCK : (b + 1) * QBLOCK] = value
            held[k, 0, 0:SUB, b * QBLOCK : (b + 1) * QBLOCK] = value[0:SUB]

    def unit_rows(r, u):
        return r * slots + u * ur

    def multiply(k):
        for r in range(4):
            for u in range(units):
                moved = dot(perm[...], held[k, r, u * 128 : (u + 1) * 128, :]).astype(BF16)
                at = unit_rows(r, u)
                for q in range(PARTS):
                    xs[at : at + ur, q * WIDE : (q + 1) * WIDE] = moved[q * ur : (q + 1) * ur]
        wg_cp[k].wait()
        wu_cp[k].wait()
        cols = pl.ds(k * CHUNK, CHUNK)
        for e in range(experts):
            for s, w in enumerate((wg, wu)):
                got = dot(xs[...], w[e, cols, :])
                if k == 0:
                    acc[e, s] = got
                else:
                    acc[e, s] += got

    exchange(chunks)
    l2, l3, l4 = lags
    flip_at = min(chunks, l4) - 1
    for step in range(chunks + l4):
        if step < chunks:
            make(step)
            exchange(step)
        if step == flip_at:
            for q in range(PARTS):
                place_t[q] = place[q].astype(F32).T.astype(BF16)
        if step == l2:
            spread(chunks)
        if 0 <= step - l2 < chunks:
            spread(step - l2)
        if step == l3:
            forward(chunks)
        if 0 <= step - l3 < chunks:
            forward(step - l3)
        if step == l4:
            arrived(chunks)
            for r in range(4):
                for u in range(units):
                    moved = dot(perm[...], wheld[r, u * 128 : (u + 1) * 128, :])
                    at = unit_rows(r, u)
                    wcol[at : at + ur, :] = moved[0:ur]
        if 0 <= step - l4 < chunks:
            arrived(step - l4)
            multiply(step - l4)

    for e in range(experts):
        gate = acc[e, 0]
        hidden[e] = (gate / (1.0 + jnp.exp(-gate)) * acc[e, 1]).astype(BF16)

    def down(k):
        wd_cp[k].wait()
        for r in range(4):
            at = pl.ds(r * slots, slots)
            total = jnp.zeros((slots, CHUNK), F32)
            for e in range(experts):
                got = dot(hidden[e, at, :], wd[e, :, k * CHUNK : (k + 1) * CHUNK])
                total += wcol[at, e : e + 1] * got
            part[k, r] = total.astype(BF16)
        remote(part.at[k, 3, pl.ds(0, half)], relay_a.at[k], 10, 11, k, at_y)
        remote(part.at[k, 3, pl.ds(half, half)], relay_b.at[k], 12, 13, k, at_x)

    def merge(k):
        wait(relay_a.at[k], 11, k)
        part[k, 1, 0:half] = (part[k, 1, 0:half].astype(F32) + relay_a[k].astype(F32)).astype(BF16)
        remote(part.at[k, 1], got_x.at[k], 14, 15, k, at_x)
        wait(relay_b.at[k], 13, k)
        part[k, 2, half:slots] = (
            part[k, 2, half:slots].astype(F32) + relay_b[k].astype(F32)
        ).astype(BF16)
        remote(part.at[k, 2], got_y.at[k], 16, 17, k, at_y)

    def home(k):
        wait(got_x.at[k], 15, k)
        wait(got_y.at[k], 17, k)
        for u in range(units):
            at = pl.ds(u * ur, ur)
            total = (
                part[k, 0, at].astype(F32) + got_x[k, at].astype(F32) + got_y[k, at].astype(F32)
            ).astype(BF16)
            stacked = jnp.concatenate(
                [total[:, q * WIDE : (q + 1) * WIDE] for q in range(PARTS)], axis=0
            )
            moved = dot(perm_t[...], stacked).astype(BF16)
            back_s[k, u * 128 : (u + 1) * 128] = moved
            if u == 0:
                back[k, 0:SUB] = moved[0:SUB]
        for j in range(1, groups):
            at = pl.ds(j * SUB, SUB)
            remote(back_s.at[k, at], back.at[k, at], 18, 19, k, at_z[j])

    out_cp = [
        pltpu.make_async_copy(obuf.at[k], out_hbm.at[:, pl.ds(k * CHUNK, CHUNK)], lsems.at[4, k])
        for k in range(chunks)
    ]

    def finish(k):
        wait(back.at[k, pl.ds(SUB, subs - SUB)], 19, k)
        for q in range(PARTS):
            obuf[k, :, q * WIDE : (q + 1) * WIDE] = dot(place_t[q], back[k]).astype(BF16)
        out_cp[k].start()

    for step in range(chunks + l4):
        if step < chunks:
            down(step)
        if 0 <= step - l2 < chunks:
            merge(step - l2)
        if 0 <= step - l3 < chunks:
            home(step - l3)
        if 0 <= step - l4 < chunks:
            finish(step - l4)

    for k in range(chunks + 1):
        src, dst = views(k)
        wait(src.at[pl.ds(SUB, subs - SUB)], 0, k)
        wait(dst.at[0], 2, k)
        wait(dst.at[0], 4, k)
        wait(dst.at[1, pl.ds(0, shalf)], 6, k)
        wait(dst.at[2, pl.ds(shalf, shalf)], 8, k)
    for k in range(chunks):
        wait(relay_a.at[k], 10, k)
        wait(relay_b.at[k], 12, k)
        wait(got_x.at[k], 14, k)
        wait(got_y.at[k], 16, k)
        wait(back_s.at[k, pl.ds(SUB, subs - SUB)], 18, k)
        out_cp[k].wait()


LAGS = (3, 6, 9)


def shards(tokens, expert_ids, route_weight, w_gate, w_up, w_down):
    groups = lax.axis_size("torus")
    rows, width = tokens.shape
    experts, _, units = w_gate.shape
    chunks = width // CHUNK
    subs = groups * SUB
    slots = groups * CAP
    anywhere = pl.BlockSpec(memory_space=pl.ANY)
    local = pl.BlockSpec(memory_space=pltpu.VMEM)
    V = pltpu.VMEM
    return pl.pallas_call(
        functools.partial(kernel, groups, chunks, LAGS),
        out_shape=jax.ShapeDtypeStruct((rows, width), BF16),
        in_specs=[anywhere, local, local, anywhere, anywhere, anywhere],
        out_specs=anywhere,
        scratch_shapes=[
            V((rows, width), BF16),
            V(w_gate.shape, BF16),
            V(w_up.shape, BF16),
            V(w_down.shape, BF16),
            V((PARTS, subs, rows), BF16),
            V((PARTS, rows, subs), BF16),
            V((128, 128), BF16),
            V((128, 128), BF16),
            V((chunks, subs, WIDE), BF16),
            V((chunks, 4, subs, WIDE), BF16),
            V((subs, 128), BF16),
            V((4, subs, 128), BF16),
            V((4 * slots, CHUNK), BF16),
            V((experts, 2, 4 * slots, units), F32),
            V((experts, 4 * slots, units), BF16),
            V((4 * slots, 128), F32),
            V((chunks, 4, slots, CHUNK), BF16),
            V((chunks, slots // 2, CHUNK), BF16),
            V((chunks, slots // 2, CHUNK), BF16),
            V((chunks, slots, CHUNK), BF16),
            V((chunks, slots, CHUNK), BF16),
            V((chunks, subs, WIDE), BF16),
            V((chunks, subs, WIDE), BF16),
            V((chunks, rows, CHUNK), BF16),
            pltpu.SemaphoreType.DMA((20, chunks + 1)),
            pltpu.SemaphoreType.DMA((5, chunks)),
        ],
        compiler_params=pltpu.CompilerParams(
            collective_id=0, has_side_effects=True, vmem_limit_bytes=64000000
        ),
    )(tokens, expert_ids.T, route_weight.T, w_gate, w_up, w_down)


def solution(mesh):
    placed = (
        P(("node", "torus"), None),
        P(("node", "torus"), None),
        P(("node", "torus"), None),
        P("torus", None, "node"),
        P("torus", None, "node"),
        P("torus", "node", None),
    )
    return jax.shard_map(
        shards, mesh=mesh, in_specs=placed, out_specs=P(("node", "torus"), None), check_vma=False
    )
```
